128 devices in a mesh: gy: 32 (over z, y_hi, x), gx: 4 (over y_lo, core).
Axes of the slice: x: 4, y: 4 (y_hi: 2, y_lo: 2; y = y_hi * 2 + y_lo), z: 4, core: 2. Of those that a mesh axis runs over, the one named last changes fastest.
Arguments:
- tall_factor: bfloat16 [32768, 8192], P('gy', 'gx'), may hold values from -6 to 6
- wide_factor: bfloat16 [8192, 4096], P('gy', 'gx'), may hold values from -0.0625 to 0.0625
- target: float32 [32768, 4096], P('gy', 'gx'), may hold values from -6 to 6
Outputs:
- product_sum: float32 [32768, 4096], P('gy', 'gx')
The draws below stay inside these ranges and needn't reach their ends.
All inputs are finite; a program needn't handle non-finite values.
Results may differ from the reference program's by a relative error of at most 0.0003.
Values may be sent and summed in bfloat16 or wider, within the bound.
No kernel may reach another device: no remote copies, remote signals or barrier semaphores. Data moves between devices by JAX's collectives and lax.ppermute only.
A program may use at most 128 MiB of HBM per device.

```python
import jax
import jax.numpy as jnp
from jax import lax

ROWS = 32768
COLS = 4096
INNER = 8192


def level_of(rng, extent, shards, least, top_value):
    def one(position, shards_of):
        heights = jax.random.uniform(jax.random.fold_in(jax.random.fold_in(rng, 6), position), (shards_of,), jnp.float32, least / len(shards), top_value / len(shards))
        return jnp.repeat(jnp.exp(heights), extent[position] // shards_of).reshape((-1,) + (1,) * (len(extent) - position - 1))

    gain = one(*shards[0])
    for cut in shards[1:]:
        gain = gain * one(*cut)
    return gain


def scatter_about(stream_key, extent, scale, most, split=(), held_as=jnp.bfloat16):
    entries = scale * jax.random.normal(stream_key, extent, jnp.float32)
    if split:
        entries = entries * level_of(stream_key, extent, split, -0.22, 0.18)
    return jnp.clip(entries, -most, most).astype(held_as)


def setup_inputs(seed: int = 0) -> dict:
    key_list = jax.random.split(jax.random.key(seed), 4)
    return {
        "tall_factor": scatter_about(key_list[0], (ROWS, INNER), 1.0, 6.0, ((0, 32), (1, 4))),
        "wide_factor": scatter_about(key_list[1], (INNER, COLS), INNER ** -0.5, 0.0625, ((0, 32), (1, 4))),
        "target": scatter_about(key_list[2], (ROWS, COLS), 1.0, 6.0, ((0, 32), (1, 4)), jnp.float32),
    }


def reference(tall_factor, wide_factor, target):
    product_sum = target - jnp.dot(tall_factor, wide_factor, preferred_element_type=jnp.float32)
    row_power = lax.optimization_barrier(jnp.sum(product_sum * product_sum, axis=1))
    product_sum = product_sum * lax.rsqrt(row_power / COLS + 1e-06)[:, None]
    return product_sum
```

```python
import functools

import jax
import jax.numpy as jnp
from jax import lax
from jax.experimental import pallas as pl
from jax.experimental.pallas import tpu as pltpu
from jax.sharding import PartitionSpec as P


AXES = ("gy", "gx")
CHUNKS = (512, 256, 128, 128)
VMEM = pl.BlockSpec(memory_space=pltpu.VMEM)
ANY = pl.BlockSpec(memory_space=pl.ANY)


def fetched(value, dz=0, dyh=0, dx=0, dyl=0, dc=0):
    pairs = []
    for place in range(128):
        gy, gx = divmod(place, 4)
        z, yh, x = gy // 8, gy // 4 % 2, gy % 4
        yl, core = gx // 2, gx % 2
        z, yh, x = (z + dz) % 4, (yh + dyh) % 2, (x + dx) % 4
        yl, core = (yl + dyl) % 2, (core + dc) % 2
        pairs.append((((z * 2 + yh) * 4 + x) * 4 + yl * 2 + core, place))
    return lax.ppermute(value, AXES, pairs)


def position():
    gy = lax.axis_index("gy")
    return gy // 8, gy // 4 % 2, gy % 4


def first_stage(block):
    half = block.shape[1] // 2
    a, b = block[:, :half], block[:, half:]
    a1, b1 = fetched(a, dz=1), fetched(b, dx=1)
    a3, b3 = fetched(a, dz=-1), fetched(b, dx=-1)
    a2, b2 = fetched(a, dz=2), fetched(b, dx=2)
    return jnp.concatenate([a, a1, a2, a3]), jnp.concatenate([b, b1, b2, b3])


def second_stage(a, b):
    half = a.shape[0] // 2
    a1, b1 = fetched(a, dx=1), fetched(b, dz=1)
    a3, b3 = fetched(a, dx=-1), fetched(b, dz=-1)
    a2t, b2t = fetched(a1[:half], dx=1), fetched(b1[:half], dz=1)
    a2b, b2b = fetched(a3[half:], dx=-1), fetched(b3[half:], dz=-1)
    return a, a1, a2t, a2b, a3, b, b1, b2t, b2b, b3


def joined_kernel(*refs):
    *parts, out, sem = refs
    rows, half = 256, 512
    z, _, x = position()
    left, right = parts[:5], parts[5:]

    def piece(group, i, j):
        if i == 2:
            return group[2 if j < 2 else 3].at[pl.ds(j % 2 * rows, rows)]
        return group[(0, 1, None, 4)[i]].at[pl.ds(j * rows, rows)]

    for i in range(4):
        for j in range(4):
            for side, group in enumerate((left, right)):
                dz, dx = (j, i) if side == 0 else (i, j)
                at = (lax.rem(z + dz, 4) * 4 + lax.rem(x + dx, 4)) * rows
                at = pl.multiple_of(at, rows)
                pltpu.make_async_copy(
                    piece(group, i, j),
                    out.at[pl.ds(at, rows), pl.ds(side * half, half)],
                    sem,
                ).start()
    pltpu.make_async_copy(out, out, sem).wait()


def joined(parts):
    return pl.pallas_call(
        joined_kernel,
        out_shape=jax.ShapeDtypeStruct((4096, 1024), jnp.bfloat16),
        in_specs=[VMEM] * 10,
        out_specs=VMEM,
        scratch_shapes=[pltpu.SemaphoreType.DMA],
        compiler_params=pltpu.CompilerParams(vmem_limit_bytes=20 << 20),
        cost_estimate=pl.CostEstimate(
            flops=1 << 20, bytes_accessed=16 << 20, transcendentals=0
        ),
        name="joined",
    )(*parts)


def minus_kernel(plan, *refs):
    acc, *ops, out = refs
    z, yh, _ = position()
    gx = lax.axis_index("gx")
    for row, size, lefts, rights in plan:
        step = min(size, 256)

        def body(r, carry, row=row, step=step, lefts=lefts, rights=rights):
            at = pl.ds(pl.multiple_of(row + r * step, step), step)
            take = pl.ds(pl.multiple_of(r * step, step), step)
            total = acc[at, :]
            for ref, flip, off in lefts:
                for w, wave in rights:
                    column = pl.multiple_of((yh ^ wave) * 1024, 1024)
                    line = pl.multiple_of((gx ^ flip) * 1024, 1024)
                    here = pl.ds(pl.multiple_of(off + r * step, step), step)
                    total = total - jnp.dot(
                        ops[ref][here, pl.ds(column, 1024)],
                        ops[w][pl.ds(line, 1024), :],
                        preferred_element_type=jnp.float32,
                    )
            out[at, :] = total
            return carry

        lax.fori_loop(0, size // step, body, 0)


def minus(acc, plan, *ops, name):
    flops = sum(2 * s * 1024 * 1024 * len(l) * len(r) for _, s, l, r in plan)
    return pl.pallas_call(
        functools.partial(minus_kernel, plan),
        out_shape=jax.ShapeDtypeStruct(acc.shape, jnp.float32),
        in_specs=[VMEM] * (1 + len(ops)),
        out_specs=VMEM,
        input_output_aliases={0: 0} if name != "own0" else {},
        compiler_params=pltpu.CompilerParams(vmem_limit_bytes=20 << 20),
        cost_estimate=pl.CostEstimate(
            flops=flops, bytes_accessed=4 << 20, transcendentals=0
        ),
        name=name,
    )(acc, *ops)


def power_kernel(row, size, acc, out):
    for r in range(size // 128):
        part = jnp.zeros((128, 128), jnp.float32)
        for c in range(8):
            v = acc[pl.ds(row + r * 128, 128), pl.ds(c * 128, 128)]
            part = part + v * v
        out[:, pl.ds(r * 128, 128)] = jnp.broadcast_to(
            jnp.sum(part.T, axis=0, keepdims=True), (8, 128)
        )


def power(acc, row, size):
    return pl.pallas_call(
        functools.partial(power_kernel, row, size),
        out_shape=jax.ShapeDtypeStruct((8, size), jnp.float32),
        in_specs=[VMEM],
        out_specs=VMEM,
        compiler_params=pltpu.CompilerParams(vmem_limit_bytes=16 << 20),
        cost_estimate=pl.CostEstimate(
            flops=size * 2048, bytes_accessed=size * 4096, transcendentals=0
        ),
        name="power",
    )(acc)


def scale_kernel(row, size, acc, s0, s1, s2, s3, *rest):
    out, stage, sem = rest[-3:]
    for r in range(size // 128):
        lanes = pl.ds(r * 128, 128)
        total = s0[:, lanes] + s1[:, lanes] + s2[:, lanes] + s3[:, lanes]
        gain = lax.rsqrt(total[0:1] * (1.0 / 4096) + 1e-06)
        gain = jnp.broadcast_to(gain, (128, 128)).T
        for c in range(8):
            cols = pl.ds(c * 128, 128)
            stage[lanes, cols] = acc[pl.ds(row + r * 128, 128), cols] * gain
        pltpu.make_async_copy(
            stage.at[lanes], out.at[pl.ds(row + r * 128, 128)], sem
        ).start()
    pltpu.make_async_copy(stage, out.at[pl.ds(row, size)], sem).wait()


def scaled(acc, powers, row, size, base=None):
    more = [] if base is None else [base]
    return pl.pallas_call(
        functools.partial(scale_kernel, row, size),
        out_shape=jax.ShapeDtypeStruct(acc.shape, jnp.float32),
        in_specs=[VMEM] * 5 + [ANY] * len(more),
        out_specs=ANY,
        input_output_aliases={5: 0} if more else {},
        scratch_shapes=[
            pltpu.VMEM((size, 1024), jnp.float32),
            pltpu.SemaphoreType.DMA,
        ],
        compiler_params=pltpu.CompilerParams(vmem_limit_bytes=20 << 20),
        cost_estimate=pl.CostEstimate(
            flops=size * 1024, bytes_accessed=size * 8192, transcendentals=0
        ),
        name="scaled",
    )(acc, *powers, *more)


def powers_of(acc, row, size):
    mine = power(acc, row, size)
    return [
        mine,
        fetched(mine, dc=1),
        fetched(mine, dyl=1),
        fetched(mine, dyl=1, dc=1),
    ]


def on_device(tall_factor, wide_factor, target):
    starts = [sum(CHUNKS[:i]) for i in range(len(CHUNKS))]
    pieces = [tall_factor[s : s + n] for s, n in zip(starts, CHUNKS)]

    near = [fetched(pieces[0], dyl=1)]
    other = fetched(wide_factor, dyh=1)
    a, b = first_stage(wide_factor)
    near += [fetched(p, dyl=1) for p in pieces[1:]]
    twin = fetched(tall_factor, dc=1)
    wave0 = joined(second_stage(a, b))
    a, b = first_stage(other)
    wave1 = joined(second_stage(a, b))
    far = [fetched(p, dc=1) for p in near]

    def sides(ref, off=0):
        return ((ref, 2, 0), (ref + 1, 3, 0))

    own = ((0, 0, 0), (1, 1, 0))
    acc = minus(target, ((0, 1024, own, ((2, 0),)),), tall_factor, twin, wave0, name="own0")
    for i in (0, 1):
        acc = minus(acc, ((starts[i], CHUNKS[i], sides(0), ((2, 0),)),), near[i], far[i], wave0, name=f"near{i}")
    acc = minus(acc, ((0, 1024, own, ((2, 1),)),), tall_factor, twin, wave1, name="own1")
    for i in (0, 1):
        acc = minus(acc, ((starts[i], CHUNKS[i], sides(0), ((2, 1),)),), near[i], far[i], wave1, name=f"near{i}b")
    acc = minus(acc, ((starts[2], CHUNKS[2], sides(0), ((2, 0), (3, 1))),), near[2], far[2], wave0, wave1, name="near2")
    powers = powers_of(acc, 0, starts[3])
    out = scaled(acc, powers, 0, starts[3])
    acc = minus(acc, ((starts[3], CHUNKS[3], sides(0), ((2, 0), (3, 1))),), near[3], far[3], wave0, wave1, name="near3")
    powers = powers_of(acc, starts[3], CHUNKS[3])
    return scaled(acc, powers, starts[3], CHUNKS[3], out)


def solution(mesh):
    return jax.shard_map(
        on_device,
        mesh=mesh,
        in_specs=(P("gy", "gx"), P("gy", "gx"), P("gy", "gx")),
        out_specs=P("gy", "gx"),
        check_vma=False,
    )
```
